32 devices in a mesh: beam: 8 (over y, x, core), tm: 4 (over z).
Axes of the slice: x: 2, y: 2, z: 4, core: 2. Of those that a mesh axis runs over, the one named last changes fastest.
Arguments:
- samples: float32 [2, 18874368], P(None, ('beam', 'tm')), parts along dimension 1, may hold values from -6 to 6
- prototype: float32 [16, 4096], replicated, may hold values from -1.5 to 1.5
Outputs:
- spectra: bfloat16 [2, 6144, 4096], P(None, 'beam', 'tm'), parts along dimension 1
The draws below stay inside these ranges and needn't reach their ends.
There are 8 independent parts, one for each index of `beam`. The reference program is written for one: setup_inputs(seed, part) draws one part's arguments, and reference() takes and returns one part's arrays. A program takes and returns all parts, laid end to end along the dimension named above; an argument that names none is the same for every part. Nothing has to cross between parts.
All inputs are finite; a program needn't handle non-finite values.
Results may differ from the reference program's by a relative error of at most 0.001.
Values may be sent and summed in bfloat16 or wider, within the bound.
A program may use at most 128 MiB of HBM per device.

```python
import math
import jax
import jax.numpy as jnp

CHANNELS = 4096
TAPS = 16
HOP = 3072
FRAMES = 768
SAMPLES = 2359296


def steps_of(rng, extent, shards, low, top_value):
    factor_of = 1.0
    for axis_at, blocks in shards:
        draws = jax.random.uniform(jax.random.fold_in(jax.random.fold_in(rng, 6), axis_at), (blocks,), jnp.float32, low / len(shards), top_value / len(shards))
        factor_of = factor_of * jnp.repeat(jnp.exp(draws), extent[axis_at] // blocks).reshape((-1,) + (1,) * (len(extent) - 1 - axis_at))
    return factor_of


def noise(own_key, dims, scale, limit, shards=(), held_as=jnp.bfloat16):
    result = jax.random.normal(own_key, dims, jnp.float32) * scale
    if len(shards) > 0:
        result = steps_of(own_key, dims, shards, -0.22, 0.18) * result
    return jnp.clip(result, min=-limit, max=limit).astype(held_as)


def setup_inputs(seed: int = 0, part: int = 0) -> dict:
    key_list = jax.random.split(jax.random.key(seed), 3)
    part_keys = jax.random.split(jax.random.fold_in(key_list[2], part), 3)
    return {
        "samples": noise(part_keys[0], (2, SAMPLES), 1.0, 6.0, ((1, 4),), jnp.float32),
        "prototype": noise(key_list[1], (TAPS, CHANNELS), TAPS ** -0.5, 1.5, (), jnp.float32),
    }


def reference(samples, prototype):
    window = TAPS * CHANNELS
    zeros_front = jnp.zeros((2, window - HOP), samples.dtype)
    extended = jnp.concatenate([zeros_front, samples], axis=1)
    signal = extended[0] + 1j * extended[1]
    frame_ids = jnp.arange(FRAMES).astype(jnp.int32)
    phase_ids = jnp.arange(CHANNELS).astype(jnp.int32)
    folded = jnp.zeros((FRAMES, CHANNELS), signal.dtype)
    for tap_index in range(TAPS):
        starts = frame_ids * HOP + tap_index * CHANNELS
        index_grid = (starts[:, None] + phase_ids[None, :]).astype(jnp.int32)
        folded = folded + prototype[tap_index][None, :] * signal[index_grid]
    transformed = jnp.fft.fft(folded, axis=1)
    rotation = (frame_ids + 1) * HOP % CHANNELS
    turns = phase_ids[None, :] * rotation[:, None] % CHANNELS
    angle = 2.0 * math.pi * turns.astype(samples.dtype) / CHANNELS
    factor = (jnp.cos(angle) - 1j * jnp.sin(angle)) / math.sqrt(CHANNELS)
    spectrum = transformed * factor
    return jnp.stack([jnp.real(spectrum), jnp.imag(spectrum)]).astype(jnp.bfloat16)
```

```python
import functools
import math

import numpy as np
import jax
import jax.numpy as jnp
from jax import lax
from jax.experimental import pallas as pl
from jax.experimental.pallas import tpu as pltpu
from jax.sharding import PartitionSpec as P

CHANNELS = 4096
TAPS = 16
HOP = 3072
LANES = 128
FIRST = 128
SECOND = CHANNELS // FIRST
ROWS = 2 * CHANNELS // LANES
HOP_ROWS = 2 * HOP // LANES
RIM = TAPS * CHANNELS - HOP
RIM_ROWS = 2 * RIM // LANES
CHUNK = 16
GROUP = 8
SCALE = 2.0 ** 24
MESH = pl.DeviceIdType.MESH


def split_pair(table):
    high = np.asarray(table, np.float32).astype(jnp.bfloat16)
    low = (np.asarray(table, np.float64) - high.astype(np.float64)).astype(jnp.bfloat16)
    return high, low


def first_table():
    b1, a, d = np.meshgrid(np.arange(4), np.arange(32), np.arange(FIRST), indexing="ij")
    angle = 2 * np.pi * ((4 * a + b1) * d % FIRST) / FIRST
    cos, sin = np.cos(angle), np.sin(angle)
    table = np.zeros((4, 32, 2, 2, FIRST))
    table[:, :, 0, 0], table[:, :, 1, 0] = cos, sin
    table[:, :, 0, 1], table[:, :, 1, 1] = -sin, cos
    high, low = split_pair(table.reshape(2 * FIRST, 2 * FIRST))
    return np.concatenate([high, high, low], axis=0)


def middle_table():
    angle = 2 * np.pi * np.outer(np.arange(SECOND), np.arange(FIRST)) / CHANNELS
    return (np.stack([np.cos(angle), np.sin(angle)]) / math.sqrt(CHANNELS)).astype(np.float32)


def second_table():
    angle = 2 * np.pi * (np.outer(np.arange(SECOND), np.arange(SECOND)) % SECOND) / SECOND
    eye = np.eye(GROUP)
    both = np.stack([np.cos(angle), np.sin(angle)])
    table = np.einsum("kcm,tu->kctum", both, eye).reshape(2 * SECOND * GROUP, GROUP * SECOND)
    high, low = split_pair(table)
    return np.concatenate([high, high, low], axis=1)


def split_value(value):
    high = value.astype(jnp.bfloat16)
    low = (value - high.astype(jnp.float32)).astype(jnp.bfloat16)
    return high, low


def encode(value):
    square = (value * SCALE) * (value * SCALE)
    power = square * square
    return jnp.where(value < 0, -power, power).astype(jnp.bfloat16)


def decode(code):
    power = code.astype(jnp.float32)
    value = jnp.sqrt(jnp.sqrt(jnp.abs(power))) * (1 / SCALE)
    return jnp.where(power < 0, -value, value)


def partner(me, step, count):
    if count & (count - 1):
        return lax.rem(me + step, count)
    other = me
    bit = 1
    while bit < count:
        if step & bit:
            other = other + bit * (1 - 2 * lax.rem(me // bit, 2))
        bit *= 2
    return other


def kernel(count, frames, x_hbm, proto_hbm, one_hbm, mid_hbm, two_hbm, out_ref,
           ext, raw, spread, proto_ref, one_ref, mid_ref, two_ref, folded, lhs, rhs, staged,
           past_out, past_in, head_out, head_in, load_sems, own_sem, rim_sems, head_sems, send_sems, recv_sems):
    me = lax.axis_index("tm")
    chunks = frames // CHUNK
    local_rows = frames * HOP_ROWS
    head_rows = CHUNK * HOP_ROWS
    past_rows = RIM_ROWS - head_rows
    width = CHANNELS // count

    near_rows = 3 * head_rows

    def part(first, size):
        return x_hbm.at[pl.ds(first, size)], ext.at[pl.ds(RIM_ROWS + first, size)]

    loads = [
        pltpu.make_async_copy(source, target, load_sems.at[at])
        for at, (source, target) in enumerate((
            part(local_rows - past_rows, past_rows),
            part(0, head_rows),
            (proto_hbm, raw),
            part(head_rows, near_rows - head_rows),
            (one_hbm, one_ref),
            (mid_hbm, mid_ref),
            (two_hbm, two_ref),
            part(near_rows, local_rows - past_rows - near_rows),
        ))
    ]
    for load in loads:
        load.start()

    barrier = pltpu.get_barrier_semaphore()
    for step in range(1, count):
        pl.semaphore_signal(barrier, inc=1, device_id={"tm": partner(me, step, count)}, device_id_type=MESH)

    def past_copy():
        return pltpu.make_async_remote_copy(
            src_ref=past_out,
            dst_ref=past_in,
            send_sem=rim_sems.at[0],
            recv_sem=rim_sems.at[1],
            device_id={"tm": lax.rem(me + 1, count)},
            device_id_type=MESH,
        )

    def head_copy():
        return pltpu.make_async_remote_copy(
            src_ref=head_out,
            dst_ref=head_in,
            send_sem=head_sems.at[0],
            recv_sem=head_sems.at[1],
            device_id={"tm": lax.rem(me + count - 1, count)},
            device_id_type=MESH,
        )

    loads[0].wait()
    past_out[...] = encode(ext[pl.ds(RIM_ROWS + local_rows - past_rows, past_rows), :])
    loads[1].wait()
    head_out[...] = encode(ext[pl.ds(RIM_ROWS, head_rows), :])
    pl.semaphore_wait(barrier, count - 1)

    @pl.when(me < count - 1)
    def _():
        past_copy().start()

    @pl.when(me > 0)
    def _():
        head_copy().start()

    @pl.when(me == 0)
    def _():
        ext[pl.ds(0, RIM_ROWS), :] = jnp.zeros((RIM_ROWS, LANES), jnp.float32)

    loads[2].wait()
    for row in range(ROWS):
        spread[pl.ds(row * TAPS, TAPS), :] = raw[:, pl.ds(row // 2 * LANES, LANES)]
    for tap in range(TAPS):
        for v in range(ROWS // 8):
            proto_ref[tap, pl.ds(v * 8, 8), :] = spread[pl.ds(v * 8 * TAPS + tap, 8, stride=TAPS), :]
    loads[3].wait()
    order = sorted(range(1, count), key=lambda step: (step < count // 2, step))
    early = [step for step in order if step <= max(1, count // 2)]

    late = chunks - 2

    def chunk_of(index):
        return jnp.where(index < late, index + 2,
                         jnp.where(index == late, 1, jnp.where(index == late + 1, chunks, 0)))

    def send(chunk, step):
        to = partner(me, step, count)
        rows = pl.ds(pl.multiple_of(me * frames + chunk * CHUNK, CHUNK), CHUNK)
        pltpu.make_async_remote_copy(
            src_ref=staged.at[chunk, to],
            dst_ref=out_ref.at[:, rows, :],
            send_sem=send_sems.at[step - 1],
            recv_sem=recv_sems.at[step - 1],
            device_id={"tm": to},
            device_id_type=MESH,
        ).start()

    def chunk_step(index, carry):
        chunk = chunk_of(index)

        @pl.when(index == 1)
        def _():
            loads[7].wait()

        @pl.when(jnp.logical_and(index == late, me > 0))
        def _():
            past_copy().wait_recv()
            ext[pl.ds(head_rows, past_rows), :] = decode(past_in[...])

        @pl.when(jnp.logical_and(index == late + 1, me < count - 1))
        def _():
            head_copy().wait_recv()
            ext[pl.ds(RIM_ROWS + local_rows, head_rows), :] = decode(head_in[...])

        base = chunk * (CHUNK * HOP_ROWS)

        def fold(v, carry):
            taps = [proto_ref[tap, pl.ds(pl.multiple_of(v * 8, 8), 8), :] for tap in range(TAPS)]
            for t in range(CHUNK):
                total = None
                for tap in range(TAPS):
                    start = pl.multiple_of(base + (HOP_ROWS * t + ROWS * tap) + v * 8, 8)
                    term = taps[tap] * ext[pl.ds(start, 8), :]
                    total = term if total is None else total + term
                turn = (t + 1) * HOP % CHANNELS * 2 // LANES // 8
                place = lax.rem(v + turn, ROWS // 8)
                folded[t, pl.ds(pl.multiple_of(place * 8, 8), 8), :] = total
            return carry

        lax.fori_loop(0, ROWS // 8, fold, 0)

        @pl.when(index == 0)
        def _():
            for load in loads[4:7]:
                load.wait()

        lane = lax.broadcasted_iota(jnp.int32, (ROWS, LANES), 1)
        even = lax.rem(lane // SECOND, 2) == 0
        for pair in range(CHUNK // 2):
            one, other = folded[2 * pair], folded[2 * pair + 1]
            upper = jnp.where(even, one, pltpu.roll(other, SECOND, 1))
            lower = jnp.where(even, pltpu.roll(one, LANES - SECOND, 1), other)
            turned = jnp.concatenate([upper, lower], axis=0).T
            high, low = split_value(turned)
            for side in range(2):
                rows = pl.ds((2 * pair + side) * SECOND, SECOND)
                for half in range(2):
                    start = (2 * half + side) * SECOND
                    piece = high[start:start + SECOND]
                    lhs[rows, pl.ds(half * LANES, LANES)] = piece
                    lhs[rows, pl.ds((2 + half) * LANES, LANES)] = low[start:start + SECOND]
                    lhs[rows, pl.ds((4 + half) * LANES, LANES)] = piece

        cos, sin = mid_ref[0], mid_ref[1]
        results = []
        for group in range(CHUNK // GROUP):
            size = GROUP * SECOND
            section = jnp.dot(lhs[pl.ds(group * size, size), :], one_ref[...],
                              preferred_element_type=jnp.float32)
            for t in range(GROUP):
                real = section[t * SECOND:(t + 1) * SECOND, :FIRST]
                imag = section[t * SECOND:(t + 1) * SECOND, FIRST:]
                for half, value in enumerate((real * cos + imag * sin, imag * cos - real * sin)):
                    high, low = split_value(value)
                    columns = pl.ds(half * FIRST, FIRST)
                    rhs[group, pl.ds(t * SECOND, SECOND), columns] = high
                    rhs[group, pl.ds(size + t * SECOND, SECOND), columns] = low
                    rhs[group, pl.ds(2 * size + t * SECOND, SECOND), columns] = high
            product = jnp.dot(two_ref[...], rhs[group], preferred_element_type=jnp.float32)
            results.append((product[:size, :FIRST] + product[size:, FIRST:],
                            product[:size, FIRST:] - product[size:, :FIRST]))
        for part in range(2):
            for c in range(SECOND):
                block = jnp.concatenate(
                    [results[group][part][c * GROUP:(c + 1) * GROUP] for group in range(CHUNK // GROUP)], axis=0)
                owner, at = divmod(c * FIRST, width)
                staged[chunk, owner, part, :, pl.ds(at, FIRST)] = block.astype(jnp.bfloat16)

        for step in early:
            send(chunk, step)
        rows = pl.ds(pl.multiple_of(me * frames + chunk * CHUNK, CHUNK), CHUNK)
        pltpu.make_async_copy(staged.at[chunk, me], out_ref.at[:, rows, :], own_sem).start()
        return carry

    def late_step(index, carry):
        for step in order:
            if step not in early:
                send(chunk_of(index), step)
        return carry

    total = chunks - 1 + jnp.where(me < count - 1, 1, 0) + jnp.where(me == 0, 1, 0)
    lax.fori_loop(0, total, chunk_step, 0)
    lax.fori_loop(0, total, late_step, 0)

    @pl.when(me < count - 1)
    def _():
        past_copy().wait_send()

    @pl.when(me > 0)
    def _():
        head_copy().wait_send()

    def each_range(device, act):
        first, last = device == 0, device == count - 1
        for chosen, skip, size in (
            (first, 0, frames + CHUNK),
            (last, CHUNK, frames - CHUNK),
            (jnp.logical_not(jnp.logical_or(first, last)), CHUNK, frames),
        ):
            @pl.when(chosen)
            def _():
                act(out_ref.at[:, pl.ds(pl.multiple_of(device * frames + skip, CHUNK), size), :])

    each_range(me, lambda rows: pltpu.make_async_copy(rows, rows, own_sem).wait())
    for step in order:
        to = partner(me, step, count)
        source = to if not count & (count - 1) else lax.rem(me + count - step, count)

        def described(rows):
            return pltpu.make_async_remote_copy(
                src_ref=rows, dst_ref=rows, send_sem=send_sems.at[step - 1],
                recv_sem=recv_sems.at[step - 1], device_id={"tm": to}, device_id_type=MESH)

        each_range(me, lambda rows: described(rows).wait_send())
        each_range(source, lambda rows: described(rows).wait_recv())


def local(count, samples, prototype):
    frames = samples.shape[1] // HOP
    rows = samples.shape[1] // LANES
    interleaved = samples.reshape(2, rows, LANES).transpose(1, 0, 2).reshape(2 * rows, LANES)
    one, middle, two = first_table(), middle_table(), second_table()
    in_hbm = pl.BlockSpec(memory_space=pltpu.HBM)
    anywhere = pl.BlockSpec(memory_space=pl.ANY)
    width = CHANNELS // count
    past = RIM_ROWS - CHUNK * HOP_ROWS
    return pl.pallas_call(
        functools.partial(kernel, count, frames),
        out_shape=pltpu.VMEM((2, frames * count, width), jnp.bfloat16),
        in_specs=[in_hbm] * 5,
        out_specs=anywhere,
        scratch_shapes=[
            pltpu.VMEM((RIM_ROWS + 2 * rows + CHUNK * HOP_ROWS, LANES), jnp.float32),
            pltpu.VMEM(prototype.shape, jnp.float32),
            pltpu.VMEM((ROWS * TAPS, LANES), jnp.float32),
            pltpu.VMEM((TAPS, ROWS, LANES), jnp.float32),
            pltpu.VMEM(one.shape, one.dtype),
            pltpu.VMEM(middle.shape, middle.dtype),
            pltpu.VMEM(two.shape, two.dtype),
            pltpu.VMEM((CHUNK, ROWS, LANES), jnp.float32),
            pltpu.VMEM((CHUNK * SECOND, 6 * LANES), jnp.bfloat16),
            pltpu.VMEM((CHUNK // GROUP, 3 * GROUP * SECOND, 2 * FIRST), jnp.bfloat16),
            pltpu.VMEM((frames // CHUNK + 1, count, 2, CHUNK, width), jnp.bfloat16),
            pltpu.VMEM((past, LANES), jnp.bfloat16),
            pltpu.VMEM((past, LANES), jnp.bfloat16),
            pltpu.VMEM((CHUNK * HOP_ROWS, LANES), jnp.bfloat16),
            pltpu.VMEM((CHUNK * HOP_ROWS, LANES), jnp.bfloat16),
            pltpu.SemaphoreType.DMA((8,)),
            pltpu.SemaphoreType.DMA,
            pltpu.SemaphoreType.DMA((2,)),
            pltpu.SemaphoreType.DMA((2,)),
            pltpu.SemaphoreType.DMA((count - 1,)),
            pltpu.SemaphoreType.DMA((count - 1,)),
        ],
        compiler_params=pltpu.CompilerParams(
            collective_id=0, has_side_effects=True, vmem_limit_bytes=60300000
        ),
    )(interleaved, prototype, jnp.asarray(one), jnp.asarray(middle), jnp.asarray(two))


def solution(mesh):
    count = mesh.shape["tm"]
    placed = (P(None, ("beam", "tm")), P())
    return jax.shard_map(
        functools.partial(local, count), mesh=mesh, in_specs=placed,
        out_specs=P(None, "beam", "tm"), check_vma=False,
    )
```

```python
import functools
import math

import numpy as np
import jax
import jax.numpy as jnp
from jax import lax
from jax.experimental import pallas as pl
from jax.experimental.pallas import tpu as pltpu
from jax.sharding import PartitionSpec as P

CHANNELS = 4096
TAPS = 16
HOP = 3072
LANES = 128
FIRST = 128
SECOND = CHANNELS // FIRST
ROWS = 2 * CHANNELS // LANES
HOP_ROWS = 2 * HOP // LANES
RIM = TAPS * CHANNELS - HOP
RIM_ROWS = 2 * RIM // LANES
CHUNK = 16
GROUP = 8
EAGER = 2
SCALE = 2.0 ** 12
MESH = pl.DeviceIdType.MESH


def split_pair(table):
    high = np.asarray(table, np.float32).astype(jnp.bfloat16)
    low = (np.asarray(table, np.float64) - high.astype(np.float64)).astype(jnp.bfloat16)
    return high, low


def first_table():
    b1, a, d = np.meshgrid(np.arange(4), np.arange(32), np.arange(FIRST), indexing="ij")
    angle = 2 * np.pi * ((4 * a + b1) * d % FIRST) / FIRST
    cos, sin = np.cos(angle), np.sin(angle)
    table = np.zeros((4, 32, 2, 2, FIRST))
    table[:, :, 0, 0], table[:, :, 1, 0] = cos, sin
    table[:, :, 0, 1], table[:, :, 1, 1] = -sin, cos
    high, low = split_pair(table.reshape(2 * FIRST, 2 * FIRST))
    return np.concatenate([high, high, low], axis=0)


def middle_table():
    angle = 2 * np.pi * np.outer(np.arange(SECOND), np.arange(FIRST)) / CHANNELS
    return (np.stack([np.cos(angle), np.sin(angle)]) / math.sqrt(CHANNELS)).astype(np.float32)


def second_table():
    angle = 2 * np.pi * (np.outer(np.arange(SECOND), np.arange(SECOND)) % SECOND) / SECOND
    eye = np.eye(GROUP)
    both = np.stack([np.cos(angle), np.sin(angle)])
    table = np.einsum("kcm,tu->kctum", both, eye).reshape(2 * SECOND * GROUP, GROUP * SECOND)
    high, low = split_pair(table)
    return np.concatenate([high, high, low], axis=1)


def split_value(value):
    high = value.astype(jnp.bfloat16)
    low = (value - high.astype(jnp.float32)).astype(jnp.bfloat16)
    return high, low


def encode(value):
    power = value * SCALE
    for _ in range(3):
        power = power * power
    return jnp.where(value < 0, -power, power).astype(jnp.bfloat16)


def decode(code):
    power = code.astype(jnp.float32)
    value = jnp.abs(power)
    for _ in range(3):
        value = jnp.sqrt(value)
    value = value * (1 / SCALE)
    return jnp.where(power < 0, -value, value)


def partner(me, step, count):
    if count & (count - 1):
        return lax.rem(me + step, count)
    other = me
    bit = 1
    while bit < count:
        if step & bit:
            other = other + bit * (1 - 2 * lax.rem(me // bit, 2))
        bit *= 2
    return other


def kernel(count, frames, x_hbm, proto_hbm, one_hbm, mid_hbm, two_hbm, out_ref,
           ext, raw, spread, proto_ref, one_ref, mid_ref, two_ref, folded, lhs, rhs, staged,
           past_out, past_in, head_out, head_in, load_sems, own_sem, rim_sems, head_sems, send_sems, recv_sems):
    me = lax.axis_index("tm")
    chunks = frames // CHUNK
    local_rows = frames * HOP_ROWS
    head_rows = CHUNK * HOP_ROWS
    past_rows = RIM_ROWS - head_rows
    width = CHANNELS // count

    near_rows = 3 * head_rows

    def part(first, size):
        return x_hbm.at[pl.ds(first, size)], ext.at[pl.ds(RIM_ROWS + first, size)]

    loads = [
        pltpu.make_async_copy(source, target, load_sems.at[at])
        for at, (source, target) in enumerate((
            part(local_rows - past_rows, past_rows),
            part(0, head_rows),
            (proto_hbm, raw),
            part(head_rows, near_rows - head_rows),
            (one_hbm, one_ref),
            (mid_hbm, mid_ref),
            (two_hbm, two_ref),
            part(near_rows, local_rows - past_rows - near_rows),
        ))
    ]
    for load in loads:
        load.start()

    barrier = pltpu.get_barrier_semaphore()
    for step in range(1, count):
        pl.semaphore_signal(barrier, inc=1, device_id={"tm": partner(me, step, count)}, device_id_type=MESH)

    def past_copy():
        return pltpu.make_async_remote_copy(
            src_ref=past_out,
            dst_ref=past_in,
            send_sem=rim_sems.at[0],
            recv_sem=rim_sems.at[1],
            device_id={"tm": lax.rem(me + 1, count)},
            device_id_type=MESH,
        )

    def head_copy():
        return pltpu.make_async_remote_copy(
            src_ref=head_out,
            dst_ref=head_in,
            send_sem=head_sems.at[0],
            recv_sem=head_sems.at[1],
            device_id={"tm": lax.rem(me + count - 1, count)},
            device_id_type=MESH,
        )

    loads[0].wait()
    past_out[...] = encode(ext[pl.ds(RIM_ROWS + local_rows - past_rows, past_rows), :])
    loads[1].wait()
    head_out[...] = encode(ext[pl.ds(RIM_ROWS, head_rows), :])
    @pl.when(me == 0)
    def _():
        ext[pl.ds(0, RIM_ROWS), :] = jnp.zeros((RIM_ROWS, LANES), jnp.float32)

    loads[2].wait()
    for row in range(ROWS):
        spread[pl.ds(row * TAPS, TAPS), :] = raw[:, pl.ds(row // 2 * LANES, LANES)]
    for tap in range(TAPS):
        for v in range(ROWS // 8):
            proto_ref[tap, pl.ds(v * 8, 8), :] = spread[pl.ds(v * 8 * TAPS + tap, 8, stride=TAPS), :]
    loads[3].wait()
    order = sorted(range(1, count), key=lambda step: (step < count // 2, step))
    early = [step for step in order if step <= max(1, count // 2)]

    late = chunks - 2

    def chunk_of(index):
        return jnp.where(index < late, index + 2,
                         jnp.where(index == late, 1, jnp.where(index == late + 1, chunks, 0)))

    def send(chunk, step):
        to = partner(me, step, count)
        rows = pl.ds(pl.multiple_of(me * frames + chunk * CHUNK, CHUNK), CHUNK)
        pltpu.make_async_remote_copy(
            src_ref=staged.at[chunk, to],
            dst_ref=out_ref.at[:, rows, :],
            send_sem=send_sems.at[step - 1],
            recv_sem=recv_sems.at[step - 1],
            device_id={"tm": to},
            device_id_type=MESH,
        ).start()

    def chunk_step(index, carry):
        chunk = chunk_of(index)

        @pl.when(index == 1)
        def _():
            loads[7].wait()

        @pl.when(jnp.logical_and(index == late, me > 0))
        def _():
            past_copy().wait_recv()
            ext[pl.ds(head_rows, past_rows), :] = decode(past_in[...])

        @pl.when(jnp.logical_and(index == late + 1, me < count - 1))
        def _():
            head_copy().wait_recv()
            ext[pl.ds(RIM_ROWS + local_rows, head_rows), :] = decode(head_in[...])

        base = chunk * (CHUNK * HOP_ROWS)

        def fold(v, carry):
            taps = [proto_ref[tap, pl.ds(pl.multiple_of(v * 8, 8), 8), :] for tap in range(TAPS)]
            for t in range(CHUNK):
                total = None
                for tap in range(TAPS):
                    start = pl.multiple_of(base + (HOP_ROWS * t + ROWS * tap) + v * 8, 8)
                    term = taps[tap] * ext[pl.ds(start, 8), :]
                    total = term if total is None else total + term
                turn = (t + 1) * HOP % CHANNELS * 2 // LANES // 8
                place = lax.rem(v + turn, ROWS // 8)
                folded[t, pl.ds(pl.multiple_of(place * 8, 8), 8), :] = total
            return carry

        lax.fori_loop(0, ROWS // 8, fold, 0)

        @pl.when(index == 0)
        def _():
            pl.semaphore_wait(barrier, count - 1)

            @pl.when(me < count - 1)
            def _():
                past_copy().start()

            @pl.when(me > 0)
            def _():
                head_copy().start()

            for load in loads[4:7]:
                load.wait()

        lane = lax.broadcasted_iota(jnp.int32, (ROWS, LANES), 1)
        even = lax.rem(lane // SECOND, 2) == 0
        for pair in range(CHUNK // 2):
            one, other = folded[2 * pair], folded[2 * pair + 1]
            upper = jnp.where(even, one, pltpu.roll(other, SECOND, 1))
            lower = jnp.where(even, pltpu.roll(one, LANES - SECOND, 1), other)
            turned = jnp.concatenate([upper, lower], axis=0).T
            high, low = split_value(turned)
            for side in range(2):
                rows = pl.ds((2 * pair + side) * SECOND, SECOND)
                for half in range(2):
                    start = (2 * half + side) * SECOND
                    piece = high[start:start + SECOND]
                    lhs[rows, pl.ds(half * LANES, LANES)] = piece
                    lhs[rows, pl.ds((2 + half) * LANES, LANES)] = low[start:start + SECOND]
                    lhs[rows, pl.ds((4 + half) * LANES, LANES)] = piece

        cos, sin = mid_ref[0], mid_ref[1]
        results = []
        for group in range(CHUNK // GROUP):
            size = GROUP * SECOND
            section = jnp.dot(lhs[pl.ds(group * size, size), :], one_ref[...],
                              preferred_element_type=jnp.float32)
            for t in range(GROUP):
                real = section[t * SECOND:(t + 1) * SECOND, :FIRST]
                imag = section[t * SECOND:(t + 1) * SECOND, FIRST:]
                for half, value in enumerate((real * cos + imag * sin, imag * cos - real * sin)):
                    high, low = split_value(value)
                    columns = pl.ds(half * FIRST, FIRST)
                    rhs[group, pl.ds(t * SECOND, SECOND), columns] = high
                    rhs[group, pl.ds(size + t * SECOND, SECOND), columns] = low
                    rhs[group, pl.ds(2 * size + t * SECOND, SECOND), columns] = high
            product = jnp.dot(two_ref[...], rhs[group], preferred_element_type=jnp.float32)
            results.append((product[:size, :FIRST] + product[size:, FIRST:],
                            product[:size, FIRST:] - product[size:, :FIRST]))
        for part in range(2):
            for c in range(SECOND):
                block = jnp.concatenate(
                    [results[group][part][c * GROUP:(c + 1) * GROUP] for group in range(CHUNK // GROUP)], axis=0)
                owner, at = divmod(c * FIRST, width)
                staged[chunk, owner, part, :, pl.ds(at, FIRST)] = block.astype(jnp.bfloat16)

        for step in early:
            send(chunk, step)

        @pl.when(index < EAGER)
        def _():
            for step in order:
                if step not in early:
                    send(chunk, step)

        rows = pl.ds(pl.multiple_of(me * frames + chunk * CHUNK, CHUNK), CHUNK)
        pltpu.make_async_copy(staged.at[chunk, me], out_ref.at[:, rows, :], own_sem).start()
        return carry

    def late_step(index, carry):
        for step in order:
            if step not in early:
                send(chunk_of(index), step)
        return carry

    total = chunks - 1 + jnp.where(me < count - 1, 1, 0) + jnp.where(me == 0, 1, 0)
    lax.fori_loop(0, total, chunk_step, 0)
    lax.fori_loop(EAGER, total, late_step, 0)

    @pl.when(me < count - 1)
    def _():
        past_copy().wait_send()

    @pl.when(me > 0)
    def _():
        head_copy().wait_send()

    def each_range(device, act):
        first, last = device == 0, device == count - 1
        for chosen, skip, size in (
            (first, 0, frames + CHUNK),
            (last, CHUNK, frames - CHUNK),
            (jnp.logical_not(jnp.logical_or(first, last)), CHUNK, frames),
        ):
            @pl.when(chosen)
            def _():
                act(out_ref.at[:, pl.ds(pl.multiple_of(device * frames + skip, CHUNK), size), :])

    each_range(me, lambda rows: pltpu.make_async_copy(rows, rows, own_sem).wait())
    for step in order:
        to = partner(me, step, count)
        source = to if not count & (count - 1) else lax.rem(me + count - step, count)

        def described(rows):
            return pltpu.make_async_remote_copy(
                src_ref=rows, dst_ref=rows, send_sem=send_sems.at[step - 1],
                recv_sem=recv_sems.at[step - 1], device_id={"tm": to}, device_id_type=MESH)

        each_range(me, lambda rows: described(rows).wait_send())
        each_range(source, lambda rows: described(rows).wait_recv())


def local(count, samples, prototype):
    frames = samples.shape[1] // HOP
    rows = samples.shape[1] // LANES
    interleaved = samples.reshape(2, rows, LANES).transpose(1, 0, 2).reshape(2 * rows, LANES)
    one, middle, two = first_table(), middle_table(), second_table()
    in_hbm = pl.BlockSpec(memory_space=pltpu.HBM)
    anywhere = pl.BlockSpec(memory_space=pl.ANY)
    width = CHANNELS // count
    past = RIM_ROWS - CHUNK * HOP_ROWS
    return pl.pallas_call(
        functools.partial(kernel, count, frames),
        out_shape=pltpu.VMEM((2, frames * count, width), jnp.bfloat16),
        in_specs=[in_hbm] * 5,
        out_specs=anywhere,
        scratch_shapes=[
            pltpu.VMEM((RIM_ROWS + 2 * rows + CHUNK * HOP_ROWS, LANES), jnp.float32),
            pltpu.VMEM(prototype.shape, jnp.float32),
            pltpu.VMEM((ROWS * TAPS, LANES), jnp.float32),
            pltpu.VMEM((TAPS, ROWS, LANES), jnp.float32),
            pltpu.VMEM(one.shape, one.dtype),
            pltpu.VMEM(middle.shape, middle.dtype),
            pltpu.VMEM(two.shape, two.dtype),
            pltpu.VMEM((CHUNK, ROWS, LANES), jnp.float32),
            pltpu.VMEM((CHUNK * SECOND, 6 * LANES), jnp.bfloat16),
            pltpu.VMEM((CHUNK // GROUP, 3 * GROUP * SECOND, 2 * FIRST), jnp.bfloat16),
            pltpu.VMEM((frames // CHUNK + 1, count, 2, CHUNK, width), jnp.bfloat16),
            pltpu.VMEM((past, LANES), jnp.bfloat16),
            pltpu.VMEM((past, LANES), jnp.bfloat16),
            pltpu.VMEM((CHUNK * HOP_ROWS, LANES), jnp.bfloat16),
            pltpu.VMEM((CHUNK * HOP_ROWS, LANES), jnp.bfloat16),
            pltpu.SemaphoreType.DMA((8,)),
            pltpu.SemaphoreType.DMA,
            pltpu.SemaphoreType.DMA((2,)),
            pltpu.SemaphoreType.DMA((2,)),
            pltpu.SemaphoreType.DMA((count - 1,)),
            pltpu.SemaphoreType.DMA((count - 1,)),
        ],
        compiler_params=pltpu.CompilerParams(
            collective_id=0, has_side_effects=True, vmem_limit_bytes=60300000
        ),
    )(interleaved, prototype, jnp.asarray(one), jnp.asarray(middle), jnp.asarray(two))


def solution(mesh):
    count = mesh.shape["tm"]
    placed = (P(None, ("beam", "tm")), P())
    return jax.shard_map(
        functools.partial(local, count), mesh=mesh, in_specs=placed,
        out_specs=P(None, "beam", "tm"), check_vma=False,
    )
```

```python
import functools
import math

import numpy as np
import jax
import jax.numpy as jnp
from jax import lax
from jax.experimental import pallas as pl
from jax.experimental.pallas import tpu as pltpu
from jax.sharding import PartitionSpec as P

CHANNELS = 4096
TAPS = 16
HOP = 3072
LANES = 128
FIRST = 128
SECOND = CHANNELS // FIRST
ROWS = 2 * CHANNELS // LANES
HOP_ROWS = 2 * HOP // LANES
RIM = TAPS * CHANNELS - HOP
RIM_ROWS = 2 * RIM // LANES
CHUNK = 8
HEAD = 16
GROUP = 8
EAGER = 12
SCALE = 2.0 ** 12
MESH = pl.DeviceIdType.MESH


def split_pair(table):
    high = np.asarray(table, np.float32).astype(jnp.bfloat16)
    low = (np.asarray(table, np.float64) - high.astype(np.float64)).astype(jnp.bfloat16)
    return high, low


def first_table():
    b1, a, d = np.meshgrid(np.arange(4), np.arange(32), np.arange(FIRST), indexing="ij")
    angle = 2 * np.pi * ((4 * a + b1) * d % FIRST) / FIRST
    cos, sin = np.cos(angle), np.sin(angle)
    table = np.zeros((4, 32, 2, 2, FIRST))
    table[:, :, 0, 0], table[:, :, 1, 0] = cos, sin
    table[:, :, 0, 1], table[:, :, 1, 1] = -sin, cos
    high, low = split_pair(table.reshape(2 * FIRST, 2 * FIRST))
    return np.concatenate([high, high, low], axis=0)


def middle_table():
    angle = 2 * np.pi * np.outer(np.arange(SECOND), np.arange(FIRST)) / CHANNELS
    return (np.stack([np.cos(angle), np.sin(angle)]) / math.sqrt(CHANNELS)).astype(np.float32)


def second_table():
    angle = 2 * np.pi * (np.outer(np.arange(SECOND), np.arange(SECOND)) % SECOND) / SECOND
    eye = np.eye(GROUP)
    both = np.stack([np.cos(angle), np.sin(angle)])
    table = np.einsum("kcm,tu->kctum", both, eye).reshape(2 * SECOND * GROUP, GROUP * SECOND)
    high, low = split_pair(table)
    return np.concatenate([high, high, low], axis=1)


def split_value(value):
    high = value.astype(jnp.bfloat16)
    low = (value - high.astype(jnp.float32)).astype(jnp.bfloat16)
    return high, low


def encode(value):
    power = value * SCALE
    for _ in range(3):
        power = power * power
    return jnp.where(value < 0, -power, power).astype(jnp.bfloat16)


def decode(code):
    power = code.astype(jnp.float32)
    value = jnp.abs(power)
    for _ in range(3):
        value = jnp.sqrt(value)
    value = value * (1 / SCALE)
    return jnp.where(power < 0, -value, value)


def partner(me, step, count):
    if count & (count - 1):
        return lax.rem(me + step, count)
    other = me
    bit = 1
    while bit < count:
        if step & bit:
            other = other + bit * (1 - 2 * lax.rem(me // bit, 2))
        bit *= 2
    return other


def kernel(count, frames, x_hbm, proto_hbm, one_hbm, mid_hbm, two_hbm, out_ref,
           ext, raw, spread, proto_ref, one_ref, mid_ref, two_ref, folded, lhs, rhs, staged,
           past_out, past_in, head_out, head_in, load_sems, own_sem, rim_sems, head_sems, send_sems, recv_sems, relay):
    me = lax.axis_index("tm")
    chunks = frames // CHUNK
    skipped = HEAD // CHUNK
    local_rows = frames * HOP_ROWS
    chunk_rows = CHUNK * HOP_ROWS
    head_rows = HEAD * HOP_ROWS
    past_rows = RIM_ROWS - head_rows
    width = CHANNELS // count
    free_first = -(-RIM_ROWS // chunk_rows)
    near_rows = (free_first + 2) * chunk_rows - HOP_ROWS + TAPS * ROWS - RIM_ROWS
    relayed = count == 4
    inner = jnp.logical_and(me > 0, me < count - 1)

    barrier = pltpu.get_barrier_semaphore()
    if relayed:
        @pl.when(me > 0)
        def _():
            pl.semaphore_signal(barrier, inc=1, device_id={"tm": me - 1}, device_id_type=MESH)

        @pl.when(me < count - 1)
        def _():
            pl.semaphore_signal(barrier, inc=1, device_id={"tm": me + 1}, device_id_type=MESH)
    else:
        for step in range(1, count):
            pl.semaphore_signal(barrier, inc=1, device_id={"tm": partner(me, step, count)}, device_id_type=MESH)

    def part(first, size):
        return x_hbm.at[pl.ds(first, size)], ext.at[pl.ds(RIM_ROWS + first, size)]

    loads = [
        pltpu.make_async_copy(source, target, load_sems.at[at])
        for at, (source, target) in enumerate((
            part(local_rows - past_rows, past_rows),
            (proto_hbm, raw),
            part(0, near_rows),
            (one_hbm, one_ref),
            (mid_hbm, mid_ref),
            (two_hbm, two_ref),
            part(near_rows, local_rows - past_rows - near_rows),
        ))
    ]
    for load in loads:
        load.start()

    def relay_to(other):
        pl.semaphore_signal(relay, inc=1, device_id={"tm": other}, device_id_type=MESH)

    def past_copy():
        return pltpu.make_async_remote_copy(
            src_ref=past_out,
            dst_ref=past_in,
            send_sem=rim_sems.at[0],
            recv_sem=rim_sems.at[1],
            device_id={"tm": lax.rem(me + 1, count)},
            device_id_type=MESH,
        )

    def head_copy():
        return pltpu.make_async_remote_copy(
            src_ref=head_out,
            dst_ref=head_in,
            send_sem=head_sems.at[0],
            recv_sem=head_sems.at[1],
            device_id={"tm": lax.rem(me + count - 1, count)},
            device_id_type=MESH,
        )

    loads[0].wait()
    past_out[...] = encode(ext[pl.ds(RIM_ROWS + local_rows - past_rows, past_rows), :])
    @pl.when(me == 0)
    def _():
        ext[pl.ds(0, RIM_ROWS), :] = jnp.zeros((RIM_ROWS, LANES), jnp.float32)

    loads[1].wait()
    for row in range(ROWS):
        spread[pl.ds(row * TAPS, TAPS), :] = raw[:, pl.ds(row // 2 * LANES, LANES)]
    for tap in range(TAPS):
        for v in range(ROWS // 8):
            proto_ref[tap, pl.ds(v * 8, 8), :] = spread[pl.ds(v * 8 * TAPS + tap, 8, stride=TAPS), :]
    pl.semaphore_wait(barrier, jnp.where(inner, 2, 1) if relayed else count - 1)

    @pl.when(me < count - 1)
    def _():
        past_copy().start()

    if relayed:
        @pl.when(inner)
        def _():
            relay_to(me - 1)
            relay_to(me + 1)

    loads[2].wait()
    order = sorted(range(1, count), key=lambda step: (step < count // 2, step))
    early = [step for step in order if step <= max(1, count // 2)]

    free = chunks - free_first
    middle = free_first - skipped

    def chunk_of(index):
        return jnp.where(index < free, index + free_first,
                         jnp.where(index < free + middle, index - free + skipped,
                                   jnp.where(index < free + middle + skipped, index - free - middle + chunks,
                                             index - free - middle - skipped)))

    def send(chunk, step):
        to = partner(me, step, count)
        rows = pl.ds(pl.multiple_of(me * frames + chunk * CHUNK, CHUNK), CHUNK)
        pltpu.make_async_remote_copy(
            src_ref=staged.at[chunk, to],
            dst_ref=out_ref.at[:, rows, :],
            send_sem=send_sems.at[step - 1],
            recv_sem=recv_sems.at[step - 1],
            device_id={"tm": to},
            device_id_type=MESH,
        ).start()

    def chunk_step(index, carry):
        chunk = chunk_of(index)

        @pl.when(index == 2)
        def _():
            loads[6].wait()

        @pl.when(jnp.logical_and(index == free, me > 0))
        def _():
            past_copy().wait_recv()
            ext[pl.ds(head_rows, past_rows), :] = decode(past_in[...])

        @pl.when(jnp.logical_and(index == free + middle, me < count - 1))
        def _():
            head_copy().wait_recv()
            ext[pl.ds(RIM_ROWS + local_rows, head_rows), :] = decode(head_in[...])

        base = chunk * chunk_rows

        def fold(v, carry):
            taps = [proto_ref[tap, pl.ds(pl.multiple_of(v * 8, 8), 8), :] for tap in range(TAPS)]
            for t in range(CHUNK):
                total = None
                for tap in range(TAPS):
                    start = pl.multiple_of(base + (HOP_ROWS * t + ROWS * tap) + v * 8, 8)
                    term = taps[tap] * ext[pl.ds(start, 8), :]
                    total = term if total is None else total + term
                turn = (t + 1) * HOP % CHANNELS * 2 // LANES // 8
                place = lax.rem(v + turn, ROWS // 8)
                folded[t, pl.ds(pl.multiple_of(place * 8, 8), 8), :] = total
            return carry

        lax.fori_loop(0, ROWS // 8, fold, 0)

        @pl.when(index == 0)
        def _():
            for load in loads[3:6]:
                load.wait()

        lane = lax.broadcasted_iota(jnp.int32, (ROWS, LANES), 1)
        even = lax.rem(lane // SECOND, 2) == 0
        for pair in range(CHUNK // 2):
            one, other = folded[2 * pair], folded[2 * pair + 1]
            upper = jnp.where(even, one, pltpu.roll(other, SECOND, 1))
            lower = jnp.where(even, pltpu.roll(one, LANES - SECOND, 1), other)
            turned = jnp.concatenate([upper, lower], axis=0).T
            high, low = split_value(turned)
            for side in range(2):
                rows = pl.ds((2 * pair + side) * SECOND, SECOND)
                for half in range(2):
                    start = (2 * half + side) * SECOND
                    piece = high[start:start + SECOND]
                    lhs[rows, pl.ds(half * LANES, LANES)] = piece
                    lhs[rows, pl.ds((2 + half) * LANES, LANES)] = low[start:start + SECOND]
                    lhs[rows, pl.ds((4 + half) * LANES, LANES)] = piece

        cos, sin = mid_ref[0], mid_ref[1]
        results = []
        for group in range(CHUNK // GROUP):
            size = GROUP * SECOND
            section = jnp.dot(lhs[pl.ds(group * size, size), :], one_ref[...],
                              preferred_element_type=jnp.float32)
            for t in range(GROUP):
                real = section[t * SECOND:(t + 1) * SECOND, :FIRST]
                imag = section[t * SECOND:(t + 1) * SECOND, FIRST:]
                for half, value in enumerate((real * cos + imag * sin, imag * cos - real * sin)):
                    high, low = split_value(value)
                    columns = pl.ds(half * FIRST, FIRST)
                    rhs[group, pl.ds(t * SECOND, SECOND), columns] = high
                    rhs[group, pl.ds(size + t * SECOND, SECOND), columns] = low
                    rhs[group, pl.ds(2 * size + t * SECOND, SECOND), columns] = high
            product = jnp.dot(two_ref[...], rhs[group], preferred_element_type=jnp.float32)
            results.append((product[:size, :FIRST] + product[size:, FIRST:],
                            product[:size, FIRST:] - product[size:, :FIRST]))
        for part in range(2):
            for c in range(SECOND):
                block = jnp.concatenate(
                    [results[group][part][c * GROUP:(c + 1) * GROUP] for group in range(CHUNK // GROUP)], axis=0)
                owner, at = divmod(c * FIRST, width)
                staged[chunk, owner, part, :, pl.ds(at, FIRST)] = block.astype(jnp.bfloat16)

        if relayed:
            @pl.when(jnp.logical_and(index < EAGER, inner))
            def _():
                send(chunk, 3)

            @pl.when(index == 0)
            def _():
                pl.semaphore_wait(relay, 1)

                @pl.when(inner)
                def _():
                    relay_to(jnp.where(me == 1, 0, count - 1))

            send(chunk, 2)
            send(chunk, 1)
        else:
            for step in early:
                send(chunk, step)

        @pl.when(jnp.logical_and(index == 0, me > 0))
        def _():
            head_out[...] = encode(ext[pl.ds(RIM_ROWS, head_rows), :])
            head_copy().start()

        rows = pl.ds(pl.multiple_of(me * frames + chunk * CHUNK, CHUNK), CHUNK)
        pltpu.make_async_copy(staged.at[chunk, me], out_ref.at[:, rows, :], own_sem).start()
        return carry

    def late_step(index, carry):
        for step in order:
            if step not in early:
                send(chunk_of(index), step)
        return carry

    total = free + middle + jnp.where(me < count - 1, skipped, 0) + jnp.where(me == 0, skipped, 0)
    lax.fori_loop(0, total, chunk_step, 0)
    if relayed:
        @pl.when(jnp.logical_not(inner))
        def _():
            pl.semaphore_wait(relay, 1)

    lax.fori_loop(jnp.where(inner, EAGER, 0) if relayed else 0, total, late_step, 0)

    @pl.when(me < count - 1)
    def _():
        past_copy().wait_send()

    @pl.when(me > 0)
    def _():
        head_copy().wait_send()

    def each_range(device, act):
        first, last = device == 0, device == count - 1
        for chosen, skip, size in (
            (first, 0, frames + HEAD),
            (last, HEAD, frames - HEAD),
            (jnp.logical_not(jnp.logical_or(first, last)), HEAD, frames),
        ):
            @pl.when(chosen)
            def _():
                act(out_ref.at[:, pl.ds(pl.multiple_of(device * frames + skip, CHUNK), size), :])

    each_range(me, lambda rows: pltpu.make_async_copy(rows, rows, own_sem).wait())
    for step in order:
        to = partner(me, step, count)
        source = to if not count & (count - 1) else lax.rem(me + count - step, count)

        def described(rows):
            return pltpu.make_async_remote_copy(
                src_ref=rows, dst_ref=rows, send_sem=send_sems.at[step - 1],
                recv_sem=recv_sems.at[step - 1], device_id={"tm": to}, device_id_type=MESH)

        each_range(me, lambda rows: described(rows).wait_send())
        each_range(source, lambda rows: described(rows).wait_recv())


def local(count, samples, prototype):
    frames = samples.shape[1] // HOP
    rows = samples.shape[1] // LANES
    interleaved = samples.reshape(2, rows, LANES).transpose(1, 0, 2).reshape(2 * rows, LANES)
    one, middle, two = first_table(), middle_table(), second_table()
    in_hbm = pl.BlockSpec(memory_space=pltpu.HBM)
    anywhere = pl.BlockSpec(memory_space=pl.ANY)
    width = CHANNELS // count
    past = RIM_ROWS - HEAD * HOP_ROWS
    return pl.pallas_call(
        functools.partial(kernel, count, frames),
        out_shape=pltpu.VMEM((2, frames * count, width), jnp.bfloat16),
        in_specs=[in_hbm] * 5,
        out_specs=anywhere,
        scratch_shapes=[
            pltpu.VMEM((RIM_ROWS + 2 * rows + HEAD * HOP_ROWS, LANES), jnp.float32),
            pltpu.VMEM(prototype.shape, jnp.float32),
            pltpu.VMEM((ROWS * TAPS, LANES), jnp.float32),
            pltpu.VMEM((TAPS, ROWS, LANES), jnp.float32),
            pltpu.VMEM(one.shape, one.dtype),
            pltpu.VMEM(middle.shape, middle.dtype),
            pltpu.VMEM(two.shape, two.dtype),
            pltpu.VMEM((CHUNK, ROWS, LANES), jnp.float32),
            pltpu.VMEM((CHUNK * SECOND, 6 * LANES), jnp.bfloat16),
            pltpu.VMEM((CHUNK // GROUP, 3 * GROUP * SECOND, 2 * FIRST), jnp.bfloat16),
            pltpu.VMEM(((frames + HEAD) // CHUNK, count, 2, CHUNK, width), jnp.bfloat16),
            pltpu.VMEM((past, LANES), jnp.bfloat16),
            pltpu.VMEM((past, LANES), jnp.bfloat16),
            pltpu.VMEM((HEAD * HOP_ROWS, LANES), jnp.bfloat16),
            pltpu.VMEM((HEAD * HOP_ROWS, LANES), jnp.bfloat16),
            pltpu.SemaphoreType.DMA((7,)),
            pltpu.SemaphoreType.DMA,
            pltpu.SemaphoreType.DMA((2,)),
            pltpu.SemaphoreType.DMA((2,)),
            pltpu.SemaphoreType.DMA((count - 1,)),
            pltpu.SemaphoreType.DMA((count - 1,)),
            pltpu.SemaphoreType.REGULAR,
        ],
        compiler_params=pltpu.CompilerParams(
            collective_id=0, has_side_effects=True, vmem_limit_bytes=60300000
        ),
    )(interleaved, prototype, jnp.asarray(one), jnp.asarray(middle), jnp.asarray(two))


def solution(mesh):
    count = mesh.shape["tm"]
    placed = (P(None, ("beam", "tm")), P())
    return jax.shard_map(
        functools.partial(local, count), mesh=mesh, in_specs=placed,
        out_specs=P(None, "beam", "tm"), check_vma=False,
    )
```

```python
import functools
import math

import numpy as np
import jax
import jax.numpy as jnp
from jax import lax
from jax.experimental import pallas as pl
from jax.experimental.pallas import tpu as pltpu
from jax.sharding import PartitionSpec as P

CHANNELS = 4096
TAPS = 16
HOP = 3072
LANES = 128
FIRST = 128
SECOND = CHANNELS // FIRST
ROWS = 2 * CHANNELS // LANES
HOP_ROWS = 2 * HOP // LANES
RIM = TAPS * CHANNELS - HOP
RIM_ROWS = 2 * RIM // LANES
CHUNK = 8
HEAD = 16
GROUP = 8
EAGER = 15
LAST = 8
HELD = 6
SCALE = 2.0 ** 12
MESH = pl.DeviceIdType.MESH


def split_pair(table):
    high = np.asarray(table, np.float32).astype(jnp.bfloat16)
    low = (np.asarray(table, np.float64) - high.astype(np.float64)).astype(jnp.bfloat16)
    return high, low


def first_table():
    b1, a, d = np.meshgrid(np.arange(4), np.arange(32), np.arange(FIRST), indexing="ij")
    angle = 2 * np.pi * ((4 * a + b1) * d % FIRST) / FIRST
    cos, sin = np.cos(angle), np.sin(angle)
    table = np.zeros((4, 32, 2, 2, FIRST))
    table[:, :, 0, 0], table[:, :, 1, 0] = cos, sin
    table[:, :, 0, 1], table[:, :, 1, 1] = -sin, cos
    high, low = split_pair(table.reshape(2 * FIRST, 2 * FIRST))
    return np.concatenate([high, high, low], axis=0)


def middle_table():
    angle = 2 * np.pi * np.outer(np.arange(SECOND), np.arange(FIRST)) / CHANNELS
    return (np.stack([np.cos(angle), np.sin(angle)]) / math.sqrt(CHANNELS)).astype(np.float32)


def second_table():
    angle = 2 * np.pi * (np.outer(np.arange(SECOND), np.arange(SECOND)) % SECOND) / SECOND
    eye = np.eye(GROUP)
    both = np.stack([np.cos(angle), np.sin(angle)])
    table = np.einsum("kcm,tu->kctum", both, eye).reshape(2 * SECOND * GROUP, GROUP * SECOND)
    high, low = split_pair(table)
    return np.concatenate([high, high, low], axis=1)


def split_value(value):
    high = value.astype(jnp.bfloat16)
    low = (value - high.astype(jnp.float32)).astype(jnp.bfloat16)
    return high, low


def encode(value):
    power = value * SCALE
    for _ in range(3):
        power = power * power
    return jnp.where(value < 0, -power, power).astype(jnp.bfloat16)


def decode(code):
    power = code.astype(jnp.float32)
    value = jnp.abs(power)
    for _ in range(3):
        value = jnp.sqrt(value)
    value = value * (1 / SCALE)
    return jnp.where(power < 0, -value, value)


def partner(me, step, count):
    if count & (count - 1):
        return lax.rem(me + step, count)
    other = me
    bit = 1
    while bit < count:
        if step & bit:
            other = other + bit * (1 - 2 * lax.rem(me // bit, 2))
        bit *= 2
    return other


def kernel(count, frames, x_hbm, proto_hbm, one_hbm, mid_hbm, two_hbm, out_ref, tail_ref,
           ext, raw, spread, proto_ref, one_ref, mid_ref, two_ref, folded, lhs, rhs, staged,
           past_out, past_in, head_out, head_in, load_sems, own_sem, rim_sems, head_sems, send_sems, recv_sems, relay):
    me = lax.axis_index("tm")
    chunks = frames // CHUNK
    skipped = HEAD // CHUNK
    local_rows = frames * HOP_ROWS
    chunk_rows = CHUNK * HOP_ROWS
    head_rows = HEAD * HOP_ROWS
    past_rows = RIM_ROWS - head_rows
    width = CHANNELS // count
    free_first = -(-RIM_ROWS // chunk_rows)
    near_rows = (free_first + 2) * chunk_rows - HOP_ROWS + TAPS * ROWS - RIM_ROWS
    relayed = count == 4
    inner = jnp.logical_and(me > 0, me < count - 1)

    barrier = pltpu.get_barrier_semaphore()
    if relayed:
        @pl.when(me > 0)
        def _():
            pl.semaphore_signal(barrier, inc=1, device_id={"tm": me - 1}, device_id_type=MESH)

        @pl.when(me < count - 1)
        def _():
            pl.semaphore_signal(barrier, inc=1, device_id={"tm": me + 1}, device_id_type=MESH)
    else:
        for step in range(1, count):
            pl.semaphore_signal(barrier, inc=1, device_id={"tm": partner(me, step, count)}, device_id_type=MESH)

    def part(first, size):
        return x_hbm.at[pl.ds(first, size)], ext.at[pl.ds(RIM_ROWS + first, size)]

    loads = [
        pltpu.make_async_copy(source, target, load_sems.at[at])
        for at, (source, target) in enumerate((
            part(local_rows - past_rows, past_rows),
            (proto_hbm, raw),
            part(0, near_rows),
            (one_hbm, one_ref),
            (mid_hbm, mid_ref),
            (two_hbm, two_ref),
            part(near_rows, local_rows - past_rows - near_rows),
        ))
    ]
    for load in loads:
        load.start()

    def relay_to(other):
        pl.semaphore_signal(relay, inc=1, device_id={"tm": other}, device_id_type=MESH)

    def past_copy():
        return pltpu.make_async_remote_copy(
            src_ref=past_out,
            dst_ref=past_in,
            send_sem=rim_sems.at[0],
            recv_sem=rim_sems.at[1],
            device_id={"tm": lax.rem(me + 1, count)},
            device_id_type=MESH,
        )

    def head_copy():
        return pltpu.make_async_remote_copy(
            src_ref=head_out,
            dst_ref=head_in,
            send_sem=head_sems.at[0],
            recv_sem=head_sems.at[1],
            device_id={"tm": lax.rem(me + count - 1, count)},
            device_id_type=MESH,
        )

    loads[0].wait()
    past_out[...] = encode(ext[pl.ds(RIM_ROWS + local_rows - past_rows, past_rows), :])
    @pl.when(me == 0)
    def _():
        ext[pl.ds(0, RIM_ROWS), :] = jnp.zeros((RIM_ROWS, LANES), jnp.float32)

    loads[1].wait()
    for row in range(ROWS):
        spread[pl.ds(row * TAPS, TAPS), :] = raw[:, pl.ds(row // 2 * LANES, LANES)]
    for tap in range(TAPS):
        for v in range(ROWS // 8):
            proto_ref[tap, pl.ds(v * 8, 8), :] = spread[pl.ds(v * 8 * TAPS + tap, 8, stride=TAPS), :]
    pl.semaphore_wait(barrier, jnp.where(inner, 2, 1) if relayed else count - 1)

    @pl.when(me < count - 1)
    def _():
        past_copy().start()

    if relayed:
        @pl.when(inner)
        def _():
            relay_to(me - 1)
            relay_to(me + 1)

    loads[2].wait()
    order = sorted(range(1, count), key=lambda step: (step < count // 2, step))
    early = [step for step in order if step <= max(1, count // 2)]

    free = chunks - free_first
    middle = free_first - skipped

    def chunk_of(index):
        return jnp.where(index < free, index + free_first,
                         jnp.where(index < free + middle, index - free + skipped,
                                   jnp.where(index < free + middle + skipped, index - free - middle + chunks,
                                             index - free - middle - skipped)))

    def send(chunk, step):
        to = partner(me, step, count)
        rows = pl.ds(pl.multiple_of(me * frames + chunk * CHUNK, CHUNK), CHUNK)
        pltpu.make_async_remote_copy(
            src_ref=staged.at[chunk, to],
            dst_ref=out_ref.at[:, rows, :],
            send_sem=send_sems.at[step - 1],
            recv_sem=recv_sems.at[step - 1],
            device_id={"tm": to},
            device_id_type=MESH,
        ).start()

    def chunk_step(index, carry):
        chunk = chunk_of(index)

        @pl.when(index == 2)
        def _():
            loads[6].wait()

        @pl.when(jnp.logical_and(index == free, me > 0))
        def _():
            past_copy().wait_recv()
            ext[pl.ds(head_rows, past_rows), :] = decode(past_in[...])

        @pl.when(jnp.logical_and(index == free + middle, me < count - 1))
        def _():
            head_copy().wait_recv()
            ext[pl.ds(RIM_ROWS + local_rows, head_rows), :] = decode(head_in[...])

        base = chunk * chunk_rows

        def fold(v, carry):
            taps = [proto_ref[tap, pl.ds(pl.multiple_of(v * 8, 8), 8), :] for tap in range(TAPS)]
            for t in range(CHUNK):
                total = None
                for tap in range(TAPS):
                    start = pl.multiple_of(base + (HOP_ROWS * t + ROWS * tap) + v * 8, 8)
                    term = taps[tap] * ext[pl.ds(start, 8), :]
                    total = term if total is None else total + term
                turn = (t + 1) * HOP % CHANNELS * 2 // LANES // 8
                place = lax.rem(v + turn, ROWS // 8)
                folded[t, pl.ds(pl.multiple_of(place * 8, 8), 8), :] = total
            return carry

        lax.fori_loop(0, ROWS // 8, fold, 0)

        @pl.when(index == 0)
        def _():
            for load in loads[3:6]:
                load.wait()

        lane = lax.broadcasted_iota(jnp.int32, (ROWS, LANES), 1)
        even = lax.rem(lane // SECOND, 2) == 0
        for pair in range(CHUNK // 2):
            one, other = folded[2 * pair], folded[2 * pair + 1]
            upper = jnp.where(even, one, pltpu.roll(other, SECOND, 1))
            lower = jnp.where(even, pltpu.roll(one, LANES - SECOND, 1), other)
            turned = jnp.concatenate([upper, lower], axis=0).T
            high, low = split_value(turned)
            for side in range(2):
                rows = pl.ds((2 * pair + side) * SECOND, SECOND)
                for half in range(2):
                    start = (2 * half + side) * SECOND
                    piece = high[start:start + SECOND]
                    lhs[rows, pl.ds(half * LANES, LANES)] = piece
                    lhs[rows, pl.ds((2 + half) * LANES, LANES)] = low[start:start + SECOND]
                    lhs[rows, pl.ds((4 + half) * LANES, LANES)] = piece

        cos, sin = mid_ref[0], mid_ref[1]
        results = []
        for group in range(CHUNK // GROUP):
            size = GROUP * SECOND
            section = jnp.dot(lhs[pl.ds(group * size, size), :], one_ref[...],
                              preferred_element_type=jnp.float32)
            for t in range(GROUP):
                real = section[t * SECOND:(t + 1) * SECOND, :FIRST]
                imag = section[t * SECOND:(t + 1) * SECOND, FIRST:]
                for half, value in enumerate((real * cos + imag * sin, imag * cos - real * sin)):
                    high, low = split_value(value)
                    columns = pl.ds(half * FIRST, FIRST)
                    rhs[group, pl.ds(t * SECOND, SECOND), columns] = high
                    rhs[group, pl.ds(size + t * SECOND, SECOND), columns] = low
                    rhs[group, pl.ds(2 * size + t * SECOND, SECOND), columns] = high
            product = jnp.dot(two_ref[...], rhs[group], preferred_element_type=jnp.float32)
            results.append((product[:size, :FIRST] + product[size:, FIRST:],
                            product[:size, FIRST:] - product[size:, :FIRST]))
        for part in range(2):
            for c in range(SECOND):
                block = jnp.concatenate(
                    [results[group][part][c * GROUP:(c + 1) * GROUP] for group in range(CHUNK // GROUP)], axis=0)
                owner, at = divmod(c * FIRST, width)
                staged[chunk, owner, part, :, pl.ds(at, FIRST)] = block.astype(jnp.bfloat16)

        if relayed:
            @pl.when(jnp.logical_and(index < EAGER, inner))
            def _():
                send(chunk, 3)

            @pl.when(index == 0)
            def _():
                pl.semaphore_wait(relay, 1)

                @pl.when(inner)
                def _():
                    relay_to(jnp.where(me == 1, 0, count - 1))

            send(chunk, 2)
            send(chunk, 1)
        else:
            for step in early:
                send(chunk, step)

        @pl.when(jnp.logical_and(index == 0, me > 0))
        def _():
            head_out[...] = encode(ext[pl.ds(RIM_ROWS, head_rows), :])
            head_copy().start()

        rows = pl.ds(pl.multiple_of(me * frames + chunk * CHUNK, CHUNK), CHUNK)
        pltpu.make_async_copy(staged.at[chunk, me], out_ref.at[:, rows, :], own_sem).start()
        return carry

    tail_first = chunks + skipped - LAST

    def late_step(index, carry):
        chunk = chunk_of(index)
        if relayed:
            @pl.when(jnp.logical_or(chunk < tail_first, jnp.logical_not(inner)))
            def _():
                send(chunk, 3)
        else:
            for step in order:
                if step not in early:
                    send(chunk, step)
        return carry

    total = free + middle + jnp.where(me < count - 1, skipped, 0) + jnp.where(me == 0, skipped, 0)
    lax.fori_loop(0, total, chunk_step, 0)
    if relayed:
        @pl.when(inner)
        def _():
            lax.fori_loop(EAGER, total, late_step, 0)
            to = partner(me, 3, count)
            for at in range(LAST):
                for part in range(2):
                    tail_ref[part, pl.ds(at * CHUNK, CHUNK), :] = staged[tail_first + at, to, part]

        @pl.when(jnp.logical_not(inner))
        def _():
            pl.semaphore_wait(relay, 1)
            lax.fori_loop(0, total - HELD, late_step, 0)
            pl.semaphore_wait(relay, 1)
            lax.fori_loop(total - HELD, total, late_step, 0)
    else:
        lax.fori_loop(0, total, late_step, 0)

    @pl.when(me < count - 1)
    def _():
        past_copy().wait_send()

    @pl.when(me > 0)
    def _():
        head_copy().wait_send()

    def each_range(device, act, left=0):
        first, last = device == 0, device == count - 1
        for chosen, skip, size in (
            (first, 0, frames + HEAD),
            (last, HEAD, frames - HEAD),
            (jnp.logical_not(jnp.logical_or(first, last)), HEAD, frames - left),
        ):
            @pl.when(chosen)
            def _():
                act(out_ref.at[:, pl.ds(pl.multiple_of(device * frames + skip, CHUNK), size), :])

    each_range(me, lambda rows: pltpu.make_async_copy(rows, rows, own_sem).wait())
    for step in order:
        to = partner(me, step, count)
        source = to if not count & (count - 1) else lax.rem(me + count - step, count)
        left = LAST * CHUNK if relayed and step == 3 else 0

        def described(rows):
            return pltpu.make_async_remote_copy(
                src_ref=rows, dst_ref=rows, send_sem=send_sems.at[step - 1],
                recv_sem=recv_sems.at[step - 1], device_id={"tm": to}, device_id_type=MESH)

        each_range(me, lambda rows: described(rows).wait_send(), left)
        if relayed and step == 2:
            @pl.when(inner)
            def _():
                relay_to(jnp.where(me == 1, 0, count - 1))

        each_range(source, lambda rows: described(rows).wait_recv(), left)


def flush(gathered_ref, out_hbm, order_ref, sems):
    order_ref[...] = jnp.zeros_like(order_ref)
    copies = [pltpu.make_async_copy(gathered_ref.at[part], out_hbm.at[part], sems.at[part]) for part in range(2)]
    for copy in copies:
        copy.start()
    for copy in copies:
        copy.wait()


def swap(count, tail_ref, order_ref, got_ref, send_sem, recv_sem):
    me = lax.axis_index("tm")

    @pl.when(jnp.logical_and(me > 0, me < count - 1))
    def _():
        other = {"tm": partner(me, 3, count)}
        barrier = pltpu.get_barrier_semaphore()
        pl.semaphore_signal(barrier, inc=1, device_id=other, device_id_type=MESH)
        pl.semaphore_wait(barrier, 1)
        copy = pltpu.make_async_remote_copy(
            src_ref=tail_ref, dst_ref=got_ref, send_sem=send_sem, recv_sem=recv_sem,
            device_id=other, device_id_type=MESH)
        copy.start()
        copy.wait()


def patch(count, frames, flushed_hbm, got_ref, out_hbm, sems):
    me = lax.axis_index("tm")

    @pl.when(jnp.logical_and(me > 0, me < count - 1))
    def _():
        size = LAST * CHUNK
        first = partner(me, 3, count) * frames + frames + HEAD - size
        rows = pl.ds(pl.multiple_of(first, CHUNK), size)
        copies = [pltpu.make_async_copy(got_ref.at[part], out_hbm.at[part, rows, :], sems.at[part]) for part in range(2)]
        for copy in copies:
            copy.start()
        for copy in copies:
            copy.wait()


def local(count, samples, prototype):
    frames = samples.shape[1] // HOP
    rows = samples.shape[1] // LANES
    interleaved = samples.reshape(2, rows, LANES).transpose(1, 0, 2).reshape(2 * rows, LANES)
    one, middle, two = first_table(), middle_table(), second_table()
    in_hbm = pl.BlockSpec(memory_space=pltpu.HBM)
    anywhere = pl.BlockSpec(memory_space=pl.ANY)
    width = CHANNELS // count
    past = RIM_ROWS - HEAD * HOP_ROWS
    whole = (2, frames * count, width)
    few = (2, LAST * CHUNK, width)
    gathered, tail = pl.pallas_call(
        functools.partial(kernel, count, frames),
        out_shape=(pltpu.VMEM(whole, jnp.bfloat16), pltpu.VMEM(few, jnp.bfloat16)),
        in_specs=[in_hbm] * 5,
        out_specs=(anywhere, pl.BlockSpec(memory_space=pltpu.VMEM)),
        scratch_shapes=[
            pltpu.VMEM((RIM_ROWS + 2 * rows + HEAD * HOP_ROWS, LANES), jnp.float32),
            pltpu.VMEM(prototype.shape, jnp.float32),
            pltpu.VMEM((ROWS * TAPS, LANES), jnp.float32),
            pltpu.VMEM((TAPS, ROWS, LANES), jnp.float32),
            pltpu.VMEM(one.shape, one.dtype),
            pltpu.VMEM(middle.shape, middle.dtype),
            pltpu.VMEM(two.shape, two.dtype),
            pltpu.VMEM((CHUNK, ROWS, LANES), jnp.float32),
            pltpu.VMEM((CHUNK * SECOND, 6 * LANES), jnp.bfloat16),
            pltpu.VMEM((CHUNK // GROUP, 3 * GROUP * SECOND, 2 * FIRST), jnp.bfloat16),
            pltpu.VMEM(((frames + HEAD) // CHUNK, count, 2, CHUNK, width), jnp.bfloat16),
            pltpu.VMEM((past, LANES), jnp.bfloat16),
            pltpu.VMEM((past, LANES), jnp.bfloat16),
            pltpu.VMEM((HEAD * HOP_ROWS, LANES), jnp.bfloat16),
            pltpu.VMEM((HEAD * HOP_ROWS, LANES), jnp.bfloat16),
            pltpu.SemaphoreType.DMA((7,)),
            pltpu.SemaphoreType.DMA,
            pltpu.SemaphoreType.DMA((2,)),
            pltpu.SemaphoreType.DMA((2,)),
            pltpu.SemaphoreType.DMA((count - 1,)),
            pltpu.SemaphoreType.DMA((count - 1,)),
            pltpu.SemaphoreType.REGULAR,
        ],
        compiler_params=pltpu.CompilerParams(
            collective_id=0, has_side_effects=True, vmem_limit_bytes=60300000
        ),
    )(interleaved, prototype, jnp.asarray(one), jnp.asarray(middle), jnp.asarray(two))
    if count != 4:
        return gathered
    small = pltpu.CompilerParams(vmem_limit_bytes=2000000)
    in_vmem = pl.BlockSpec(memory_space=pltpu.VMEM)
    flushed, ordered = pl.pallas_call(
        flush, out_shape=(pltpu.HBM(whole, jnp.bfloat16), pltpu.VMEM((8, LANES), jnp.float32)),
        in_specs=[anywhere], out_specs=(in_hbm, in_vmem),
        scratch_shapes=[pltpu.SemaphoreType.DMA((2,))], compiler_params=small,
    )(gathered)
    got = pl.pallas_call(
        functools.partial(swap, count), out_shape=pltpu.VMEM(few, jnp.bfloat16),
        in_specs=[anywhere, anywhere], out_specs=anywhere,
        scratch_shapes=[pltpu.SemaphoreType.DMA, pltpu.SemaphoreType.DMA],
        compiler_params=pltpu.CompilerParams(
            collective_id=1, has_side_effects=True, vmem_limit_bytes=2000000),
    )(tail, ordered)
    return pl.pallas_call(
        functools.partial(patch, count, frames), out_shape=pltpu.HBM(whole, jnp.bfloat16),
        in_specs=[in_hbm, anywhere], out_specs=in_hbm, input_output_aliases={0: 0},
        scratch_shapes=[pltpu.SemaphoreType.DMA((2,))], compiler_params=small,
    )(flushed, got)


def solution(mesh):
    count = mesh.shape["tm"]
    placed = (P(None, ("beam", "tm")), P())
    return jax.shard_map(
        functools.partial(local, count), mesh=mesh, in_specs=placed,
        out_specs=P(None, "beam", "tm"), check_vma=False,
    )
```

```python
import functools
import math

import numpy as np
import jax
import jax.numpy as jnp
from jax import lax
from jax.experimental import pallas as pl
from jax.experimental.pallas import tpu as pltpu
from jax.sharding import PartitionSpec as P

CHANNELS = 4096
TAPS = 16
HOP = 3072
LANES = 128
FIRST = 128
SECOND = CHANNELS // FIRST
ROWS = 2 * CHANNELS // LANES
HOP_ROWS = 2 * HOP // LANES
RIM = TAPS * CHANNELS - HOP
RIM_ROWS = 2 * RIM // LANES
CHUNK = 8
HEAD = 16
GROUP = 8
EAGER = 15
LAST = 8
HELD = (8, 6)
SCALE = 2.0 ** 12
MESH = pl.DeviceIdType.MESH


def split_pair(table):
    high = np.asarray(table, np.float32).astype(jnp.bfloat16)
    low = (np.asarray(table, np.float64) - high.astype(np.float64)).astype(jnp.bfloat16)
    return high, low


def first_table():
    b1, a, d = np.meshgrid(np.arange(4), np.arange(32), np.arange(FIRST), indexing="ij")
    angle = 2 * np.pi * ((4 * a + b1) * d % FIRST) / FIRST
    cos, sin = np.cos(angle), np.sin(angle)
    table = np.zeros((4, 32, 2, 2, FIRST))
    table[:, :, 0, 0], table[:, :, 1, 0] = cos, sin
    table[:, :, 0, 1], table[:, :, 1, 1] = -sin, cos
    high, low = split_pair(table.reshape(2 * FIRST, 2 * FIRST))
    return np.concatenate([high, high, low], axis=0)


def middle_table():
    angle = 2 * np.pi * np.outer(np.arange(SECOND), np.arange(FIRST)) / CHANNELS
    return (np.stack([np.cos(angle), np.sin(angle)]) / math.sqrt(CHANNELS)).astype(np.float32)


def second_table():
    angle = 2 * np.pi * (np.outer(np.arange(SECOND), np.arange(SECOND)) % SECOND) / SECOND
    eye = np.eye(GROUP)
    both = np.stack([np.cos(angle), np.sin(angle)])
    table = np.einsum("kcm,tu->kctum", both, eye).reshape(2 * SECOND * GROUP, GROUP * SECOND)
    high, low = split_pair(table)
    return np.concatenate([high, high, low], axis=1)


def split_value(value):
    high = value.astype(jnp.bfloat16)
    low = (value - high.astype(jnp.float32)).astype(jnp.bfloat16)
    return high, low


def encode(value):
    power = value * SCALE
    for _ in range(3):
        power = power * power
    return jnp.where(value < 0, -power, power).astype(jnp.bfloat16)


def decode(code):
    power = code.astype(jnp.float32)
    value = jnp.abs(power)
    for _ in range(3):
        value = jnp.sqrt(value)
    value = value * (1 / SCALE)
    return jnp.where(power < 0, -value, value)


def partner(me, step, count):
    if count & (count - 1):
        return lax.rem(me + step, count)
    other = me
    bit = 1
    while bit < count:
        if step & bit:
            other = other + bit * (1 - 2 * lax.rem(me // bit, 2))
        bit *= 2
    return other


def kernel(count, frames, x_hbm, proto_hbm, one_hbm, mid_hbm, two_hbm, out_ref, tail_ref,
           ext, raw, spread, proto_ref, one_ref, mid_ref, two_ref, folded, lhs, rhs, staged,
           past_out, past_in, head_out, head_in, load_sems, own_sem, rim_sems, head_sems, send_sems, recv_sems, relay):
    me = lax.axis_index("tm")
    chunks = frames // CHUNK
    skipped = HEAD // CHUNK
    local_rows = frames * HOP_ROWS
    chunk_rows = CHUNK * HOP_ROWS
    head_rows = HEAD * HOP_ROWS
    past_rows = RIM_ROWS - head_rows
    width = CHANNELS // count
    free_first = -(-RIM_ROWS // chunk_rows)
    near_rows = (free_first + 2) * chunk_rows - HOP_ROWS + TAPS * ROWS - RIM_ROWS
    relayed = count == 4
    held = jnp.where(lax.rem(lax.axis_index("beam"), 2) == 0, HELD[0], HELD[1])
    eager = EAGER - jnp.where(me == 1, lax.rem(lax.axis_index("beam"), 2), 0)
    inner = jnp.logical_and(me > 0, me < count - 1)

    barrier = pltpu.get_barrier_semaphore()
    if relayed:
        @pl.when(me > 0)
        def _():
            pl.semaphore_signal(barrier, inc=1, device_id={"tm": me - 1}, device_id_type=MESH)

        @pl.when(me < count - 1)
        def _():
            pl.semaphore_signal(barrier, inc=1, device_id={"tm": me + 1}, device_id_type=MESH)
    else:
        for step in range(1, count):
            pl.semaphore_signal(barrier, inc=1, device_id={"tm": partner(me, step, count)}, device_id_type=MESH)

    def part(first, size):
        return x_hbm.at[pl.ds(first, size)], ext.at[pl.ds(RIM_ROWS + first, size)]

    loads = [
        pltpu.make_async_copy(source, target, load_sems.at[at])
        for at, (source, target) in enumerate((
            part(local_rows - past_rows, past_rows),
            (proto_hbm, raw),
            part(0, near_rows),
            (one_hbm, one_ref),
            (mid_hbm, mid_ref),
            (two_hbm, two_ref),
            part(near_rows, local_rows - past_rows - near_rows),
        ))
    ]
    for load in loads:
        load.start()

    def relay_to(other):
        pl.semaphore_signal(relay, inc=1, device_id={"tm": other}, device_id_type=MESH)

    def past_copy():
        return pltpu.make_async_remote_copy(
            src_ref=past_out,
            dst_ref=past_in,
            send_sem=rim_sems.at[0],
            recv_sem=rim_sems.at[1],
            device_id={"tm": lax.rem(me + 1, count)},
            device_id_type=MESH,
        )

    def head_copy():
        return pltpu.make_async_remote_copy(
            src_ref=head_out,
            dst_ref=head_in,
            send_sem=head_sems.at[0],
            recv_sem=head_sems.at[1],
            device_id={"tm": lax.rem(me + count - 1, count)},
            device_id_type=MESH,
        )

    loads[0].wait()
    past_out[...] = encode(ext[pl.ds(RIM_ROWS + local_rows - past_rows, past_rows), :])
    @pl.when(me == 0)
    def _():
        ext[pl.ds(0, RIM_ROWS), :] = jnp.zeros((RIM_ROWS, LANES), jnp.float32)

    loads[1].wait()
    for row in range(ROWS):
        spread[pl.ds(row * TAPS, TAPS), :] = raw[:, pl.ds(row // 2 * LANES, LANES)]
    for tap in range(TAPS):
        for v in range(ROWS // 8):
            proto_ref[tap, pl.ds(v * 8, 8), :] = spread[pl.ds(v * 8 * TAPS + tap, 8, stride=TAPS), :]
    pl.semaphore_wait(barrier, jnp.where(inner, 2, 1) if relayed else count - 1)

    @pl.when(me < count - 1)
    def _():
        past_copy().start()

    if relayed:
        @pl.when(inner)
        def _():
            relay_to(me - 1)
            relay_to(me + 1)

    loads[2].wait()
    order = sorted(range(1, count), key=lambda step: (step < count // 2, step))
    early = [step for step in order if step <= max(1, count // 2)]

    free = chunks - free_first
    middle = free_first - skipped

    def chunk_of(index):
        return jnp.where(index < free, index + free_first,
                         jnp.where(index < free + middle, index - free + skipped,
                                   jnp.where(index < free + middle + skipped, index - free - middle + chunks,
                                             index - free - middle - skipped)))

    def send(chunk, step):
        to = partner(me, step, count)
        rows = pl.ds(pl.multiple_of(me * frames + chunk * CHUNK, CHUNK), CHUNK)
        pltpu.make_async_remote_copy(
            src_ref=staged.at[chunk, to],
            dst_ref=out_ref.at[:, rows, :],
            send_sem=send_sems.at[step - 1],
            recv_sem=recv_sems.at[step - 1],
            device_id={"tm": to},
            device_id_type=MESH,
        ).start()

    def chunk_step(index, carry):
        chunk = chunk_of(index)

        @pl.when(index == 2)
        def _():
            loads[6].wait()

        @pl.when(jnp.logical_and(index == free, me > 0))
        def _():
            past_copy().wait_recv()
            ext[pl.ds(head_rows, past_rows), :] = decode(past_in[...])

        @pl.when(jnp.logical_and(index == free + middle, me < count - 1))
        def _():
            head_copy().wait_recv()
            ext[pl.ds(RIM_ROWS + local_rows, head_rows), :] = decode(head_in[...])

        base = chunk * chunk_rows

        def fold(v, carry):
            taps = [proto_ref[tap, pl.ds(pl.multiple_of(v * 8, 8), 8), :] for tap in range(TAPS)]
            for t in range(CHUNK):
                total = None
                for tap in range(TAPS):
                    start = pl.multiple_of(base + (HOP_ROWS * t + ROWS * tap) + v * 8, 8)
                    term = taps[tap] * ext[pl.ds(start, 8), :]
                    total = term if total is None else total + term
                turn = (t + 1) * HOP % CHANNELS * 2 // LANES // 8
                place = lax.rem(v + turn, ROWS // 8)
                folded[t, pl.ds(pl.multiple_of(place * 8, 8), 8), :] = total
            return carry

        lax.fori_loop(0, ROWS // 8, fold, 0)

        @pl.when(index == 0)
        def _():
            for load in loads[3:6]:
                load.wait()

        lane = lax.broadcasted_iota(jnp.int32, (ROWS, LANES), 1)
        even = lax.rem(lane // SECOND, 2) == 0
        for pair in range(CHUNK // 2):
            one, other = folded[2 * pair], folded[2 * pair + 1]
            upper = jnp.where(even, one, pltpu.roll(other, SECOND, 1))
            lower = jnp.where(even, pltpu.roll(one, LANES - SECOND, 1), other)
            turned = jnp.concatenate([upper, lower], axis=0).T
            high, low = split_value(turned)
            for side in range(2):
                rows = pl.ds((2 * pair + side) * SECOND, SECOND)
                for half in range(2):
                    start = (2 * half + side) * SECOND
                    piece = high[start:start + SECOND]
                    lhs[rows, pl.ds(half * LANES, LANES)] = piece
                    lhs[rows, pl.ds((2 + half) * LANES, LANES)] = low[start:start + SECOND]
                    lhs[rows, pl.ds((4 + half) * LANES, LANES)] = piece

        cos, sin = mid_ref[0], mid_ref[1]
        results = []
        for group in range(CHUNK // GROUP):
            size = GROUP * SECOND
            section = jnp.dot(lhs[pl.ds(group * size, size), :], one_ref[...],
                              preferred_element_type=jnp.float32)
            for t in range(GROUP):
                real = section[t * SECOND:(t + 1) * SECOND, :FIRST]
                imag = section[t * SECOND:(t + 1) * SECOND, FIRST:]
                for half, value in enumerate((real * cos + imag * sin, imag * cos - real * sin)):
                    high, low = split_value(value)
                    columns = pl.ds(half * FIRST, FIRST)
                    rhs[group, pl.ds(t * SECOND, SECOND), columns] = high
                    rhs[group, pl.ds(size + t * SECOND, SECOND), columns] = low
                    rhs[group, pl.ds(2 * size + t * SECOND, SECOND), columns] = high
            product = jnp.dot(two_ref[...], rhs[group], preferred_element_type=jnp.float32)
            results.append((product[:size, :FIRST] + product[size:, FIRST:],
                            product[:size, FIRST:] - product[size:, :FIRST]))
        for part in range(2):
            for c in range(SECOND):
                block = jnp.concatenate(
                    [results[group][part][c * GROUP:(c + 1) * GROUP] for group in range(CHUNK // GROUP)], axis=0)
                owner, at = divmod(c * FIRST, width)
                staged[chunk, owner, part, :, pl.ds(at, FIRST)] = block.astype(jnp.bfloat16)

        if relayed:
            @pl.when(jnp.logical_and(index < eager, inner))
            def _():
                send(chunk, 3)

            @pl.when(index == 0)
            def _():
                pl.semaphore_wait(relay, 1)

                @pl.when(inner)
                def _():
                    relay_to(jnp.where(me == 1, 0, count - 1))

            send(chunk, 2)
            send(chunk, 1)
        else:
            for step in early:
                send(chunk, step)

        @pl.when(jnp.logical_and(index == 0, me > 0))
        def _():
            head_out[...] = encode(ext[pl.ds(RIM_ROWS, head_rows), :])
            head_copy().start()

        rows = pl.ds(pl.multiple_of(me * frames + chunk * CHUNK, CHUNK), CHUNK)
        pltpu.make_async_copy(staged.at[chunk, me], out_ref.at[:, rows, :], own_sem).start()
        return carry

    tail_first = chunks + skipped - LAST

    def late_step(index, carry):
        chunk = chunk_of(index)
        if relayed:
            @pl.when(jnp.logical_or(chunk < tail_first, jnp.logical_not(inner)))
            def _():
                send(chunk, 3)
        else:
            for step in order:
                if step not in early:
                    send(chunk, step)
        return carry

    total = free + middle + jnp.where(me < count - 1, skipped, 0) + jnp.where(me == 0, skipped, 0)
    lax.fori_loop(0, total, chunk_step, 0)
    if relayed:
        @pl.when(inner)
        def _():
            lax.fori_loop(eager, total, late_step, 0)
            to = partner(me, 3, count)
            for at in range(LAST):
                for part in range(2):
                    tail_ref[part, pl.ds(at * CHUNK, CHUNK), :] = staged[tail_first + at, to, part]

        @pl.when(jnp.logical_not(inner))
        def _():
            pl.semaphore_wait(relay, 1)
            lax.fori_loop(0, total - held, late_step, 0)
            pl.semaphore_wait(relay, 1)
            lax.fori_loop(total - held, total, late_step, 0)
    else:
        lax.fori_loop(0, total, late_step, 0)

    @pl.when(me < count - 1)
    def _():
        past_copy().wait_send()

    @pl.when(me > 0)
    def _():
        head_copy().wait_send()

    def each_range(device, act, left=0):
        first, last = device == 0, device == count - 1
        for chosen, skip, size in (
            (first, 0, frames + HEAD),
            (last, HEAD, frames - HEAD),
            (jnp.logical_not(jnp.logical_or(first, last)), HEAD, frames - left),
        ):
            @pl.when(chosen)
            def _():
                act(out_ref.at[:, pl.ds(pl.multiple_of(device * frames + skip, CHUNK), size), :])

    each_range(me, lambda rows: pltpu.make_async_copy(rows, rows, own_sem).wait())
    for step in order:
        to = partner(me, step, count)
        source = to if not count & (count - 1) else lax.rem(me + count - step, count)
        left = LAST * CHUNK if relayed and step == 3 else 0

        def described(rows):
            return pltpu.make_async_remote_copy(
                src_ref=rows, dst_ref=rows, send_sem=send_sems.at[step - 1],
                recv_sem=recv_sems.at[step - 1], device_id={"tm": to}, device_id_type=MESH)

        each_range(me, lambda rows: described(rows).wait_send(), left)
        if relayed and step == 2:
            @pl.when(inner)
            def _():
                relay_to(jnp.where(me == 1, 0, count - 1))

        each_range(source, lambda rows: described(rows).wait_recv(), left)


def flush(gathered_ref, out_hbm, order_ref, sems):
    order_ref[...] = jnp.zeros_like(order_ref)
    copies = [pltpu.make_async_copy(gathered_ref.at[part], out_hbm.at[part], sems.at[part]) for part in range(2)]
    for copy in copies:
        copy.start()
    for copy in copies:
        copy.wait()


def swap(count, tail_ref, order_ref, got_ref, send_sem, recv_sem):
    me = lax.axis_index("tm")

    @pl.when(jnp.logical_and(me > 0, me < count - 1))
    def _():
        other = {"tm": partner(me, 3, count)}
        barrier = pltpu.get_barrier_semaphore()
        pl.semaphore_signal(barrier, inc=1, device_id=other, device_id_type=MESH)
        pl.semaphore_wait(barrier, 1)
        copy = pltpu.make_async_remote_copy(
            src_ref=tail_ref, dst_ref=got_ref, send_sem=send_sem, recv_sem=recv_sem,
            device_id=other, device_id_type=MESH)
        copy.start()
        copy.wait()


def patch(count, frames, flushed_hbm, got_ref, out_hbm, sems):
    me = lax.axis_index("tm")

    @pl.when(jnp.logical_and(me > 0, me < count - 1))
    def _():
        size = LAST * CHUNK
        first = partner(me, 3, count) * frames + frames + HEAD - size
        rows = pl.ds(pl.multiple_of(first, CHUNK), size)
        copies = [pltpu.make_async_copy(got_ref.at[part], out_hbm.at[part, rows, :], sems.at[part]) for part in range(2)]
        for copy in copies:
            copy.start()
        for copy in copies:
            copy.wait()


def local(count, samples, prototype):
    frames = samples.shape[1] // HOP
    rows = samples.shape[1] // LANES
    interleaved = samples.reshape(2, rows, LANES).transpose(1, 0, 2).reshape(2 * rows, LANES)
    one, middle, two = first_table(), middle_table(), second_table()
    in_hbm = pl.BlockSpec(memory_space=pltpu.HBM)
    anywhere = pl.BlockSpec(memory_space=pl.ANY)
    width = CHANNELS // count
    past = RIM_ROWS - HEAD * HOP_ROWS
    whole = (2, frames * count, width)
    few = (2, LAST * CHUNK, width)
    gathered, tail = pl.pallas_call(
        functools.partial(kernel, count, frames),
        out_shape=(pltpu.VMEM(whole, jnp.bfloat16), pltpu.VMEM(few, jnp.bfloat16)),
        in_specs=[in_hbm] * 5,
        out_specs=(anywhere, pl.BlockSpec(memory_space=pltpu.VMEM)),
        scratch_shapes=[
            pltpu.VMEM((RIM_ROWS + 2 * rows + HEAD * HOP_ROWS, LANES), jnp.float32),
            pltpu.VMEM(prototype.shape, jnp.float32),
            pltpu.VMEM((ROWS * TAPS, LANES), jnp.float32),
            pltpu.VMEM((TAPS, ROWS, LANES), jnp.float32),
            pltpu.VMEM(one.shape, one.dtype),
            pltpu.VMEM(middle.shape, middle.dtype),
            pltpu.VMEM(two.shape, two.dtype),
            pltpu.VMEM((CHUNK, ROWS, LANES), jnp.float32),
            pltpu.VMEM((CHUNK * SECOND, 6 * LANES), jnp.bfloat16),
            pltpu.VMEM((CHUNK // GROUP, 3 * GROUP * SECOND, 2 * FIRST), jnp.bfloat16),
            pltpu.VMEM(((frames + HEAD) // CHUNK, count, 2, CHUNK, width), jnp.bfloat16),
            pltpu.VMEM((past, LANES), jnp.bfloat16),
            pltpu.VMEM((past, LANES), jnp.bfloat16),
            pltpu.VMEM((HEAD * HOP_ROWS, LANES), jnp.bfloat16),
            pltpu.VMEM((HEAD * HOP_ROWS, LANES), jnp.bfloat16),
            pltpu.SemaphoreType.DMA((7,)),
            pltpu.SemaphoreType.DMA,
            pltpu.SemaphoreType.DMA((2,)),
            pltpu.SemaphoreType.DMA((2,)),
            pltpu.SemaphoreType.DMA((count - 1,)),
            pltpu.SemaphoreType.DMA((count - 1,)),
            pltpu.SemaphoreType.REGULAR,
        ],
        compiler_params=pltpu.CompilerParams(
            collective_id=0, has_side_effects=True, vmem_limit_bytes=60300000
        ),
    )(interleaved, prototype, jnp.asarray(one), jnp.asarray(middle), jnp.asarray(two))
    if count != 4:
        return gathered
    small = pltpu.CompilerParams(vmem_limit_bytes=2000000)
    in_vmem = pl.BlockSpec(memory_space=pltpu.VMEM)
    flushed, ordered = pl.pallas_call(
        flush, out_shape=(pltpu.HBM(whole, jnp.bfloat16), pltpu.VMEM((8, LANES), jnp.float32)),
        in_specs=[anywhere], out_specs=(in_hbm, in_vmem),
        scratch_shapes=[pltpu.SemaphoreType.DMA((2,))], compiler_params=small,
    )(gathered)
    got = pl.pallas_call(
        functools.partial(swap, count), out_shape=pltpu.VMEM(few, jnp.bfloat16),
        in_specs=[anywhere, anywhere], out_specs=anywhere,
        scratch_shapes=[pltpu.SemaphoreType.DMA, pltpu.SemaphoreType.DMA],
        compiler_params=pltpu.CompilerParams(
            collective_id=1, has_side_effects=True, vmem_limit_bytes=2000000),
    )(tail, ordered)
    return pl.pallas_call(
        functools.partial(patch, count, frames), out_shape=pltpu.HBM(whole, jnp.bfloat16),
        in_specs=[in_hbm, anywhere], out_specs=in_hbm, input_output_aliases={0: 0},
        scratch_shapes=[pltpu.SemaphoreType.DMA((2,))], compiler_params=small,
    )(flushed, got)


def solution(mesh):
    count = mesh.shape["tm"]
    placed = (P(None, ("beam", "tm")), P())
    return jax.shard_map(
        functools.partial(local, count), mesh=mesh, in_specs=placed,
        out_specs=P(None, "beam", "tm"), check_vma=False,
    )
```
